32 devices in a mesh: pipe: 4 (over y, core), vocab: 2 (over x), expert: 4 (over z).
Axes of the slice: x: 2, y: 2, z: 4, core: 2. Of those that a mesh axis runs over, the one named last changes fastest.
Arguments:
- token_ids: int32 [192], replicated, may hold values from 0 to 65535
- routes: int32 [192, 2], replicated, may hold values from 0 to 3, all different within a row; in each aligned block of 192 rows (0 to 191, 192 to 383, ...) at most 144 rows name the same one
- gate_weights: float32 [192, 2], replicated, may hold values from 0.2 to 1
- embed_table: bfloat16 [65536, 7168], P(('pipe', 'vocab'), 'expert'), may hold values from -0.59765625 to 0.59765625
- w_gate: bfloat16 [4, 7168, 2048], P('expert', None, ('pipe', 'vocab')), may hold values from -0.5 to 0.5
- w_up: bfloat16 [4, 7168, 2048], P('expert', None, ('pipe', 'vocab')), may hold values from -0.5 to 0.5
- w_down: bfloat16 [4, 2048, 7168], P('expert', ('pipe', 'vocab')), may hold values from -0.125 to 0.125
Outputs:
- logits: bfloat16 [192, 65536], P('expert', ('pipe', 'vocab'))
The draws below stay inside these ranges and needn't reach their ends.
Inputs may be any that keep to these rules, and one draw needn't show every extreme that they name: `routes`: each row names 2 different experts; over all 192 rows no expert is named more than 144 times, a bound that some block reaches.
All inputs are finite; a program needn't handle non-finite values.
Results may differ from the reference program's by a relative error of at most 0.025.
Values may be sent and summed in bfloat16 or wider, within the bound.
A program may use at most 128 MiB of HBM per device.

```python
import math
import jax
import jax.numpy as jnp
import numpy as np
from jax import lax

D = 7168
FF = 2048
VOC = 65536
TOPK = 2
EXPERTS = 4
TOKENS = 192
CAP = 144
N_EXPERT = 4


def set_ends(entries, stream_key, smallest, largest):
    shape = entries.shape
    spot = [jax.random.randint(jax.random.fold_in(stream_key, axis), (), 0, shape[axis]) for axis in range(len(shape))]
    entries = entries.at[tuple(spot)].set(smallest)
    longest = shape.index(max(shape))
    spot[longest] = (spot[longest] + 1) % shape[longest]
    return entries.at[tuple(spot)].set(largest)


def shard_levels(key, shape, split, low, largest):
    gain, own = 1.0, jax.random.fold_in(key, 6)
    for axis_at, blocks in split:
        draws = jnp.exp(jax.random.uniform(jax.random.fold_in(own, axis_at), (blocks,), jnp.float32, low / len(split), largest / len(split)))
        gain = gain * jnp.repeat(draws, shape[axis_at] // blocks).reshape([-1 if axis == axis_at else 1 for axis in range(len(shape))])
    return gain


def cumulative_ranks(count, lean):
    weights = [(1 << 20) // math.isqrt(rank ** lean) + 1 for rank in range(1, count + 1)]
    width = 1 + sum(weights) // (1 << 30)
    return np.cumsum(np.array([max(1, weight // width) for weight in weights]))


def ranked(key, extent, count, slope):
    grid = cumulative_ranks(count, slope)
    pick = jax.random.randint(jax.random.fold_in(key, 1), extent, 0, int(grid[count - 1]))
    grade = jnp.searchsorted(jnp.asarray(grid, jnp.int32), pick, side="right")
    return jax.random.permutation(jax.random.fold_in(key, 2), count)[grade].astype(jnp.int32)


def shared_out(key, own, number, rows, amount, top, reach, slope):
    ranking = jax.random.permutation(key, amount)
    packed, usual = portions_of(amount, rows * top, reach, slope, True), portions_of(amount, rows * top, reach, slope, False)
    places = jnp.arange(amount)

    def named(tallies, turn):
        used = int((tallies > 0).sum())
        fixed = max(1, used // 4)
        passed = fixed + (places - fixed + turn * (used - fixed)) % max(1, amount - fixed)
        return jnp.zeros((amount,), jnp.int32).at[ranking[jnp.where(places < fixed, places, passed)]].set(jnp.asarray(tallies, jnp.int32))

    tallies = jnp.where(number % 4 == 0, named(packed, number // 4), named(usual, number - number // 4 - 1))
    mixed = jax.random.permutation(jax.random.fold_in(own, 3), amount)
    giver, sink = mixed[0:amount // 2 * 2:2], mixed[1:amount // 2 * 2:2]
    margin = jnp.minimum(tallies[giver] - 1, reach - tallies[sink]) // 2
    margin = jnp.where((giver == ranking[0]) | (sink == ranking[0]) | (tallies[sink] == 0), 0, jnp.maximum(margin, 0))
    passed = jax.random.randint(jax.random.fold_in(own, 4), (amount // 2,), 0, 1 << 20) % (margin + 1)
    tallies = tallies.at[giver].add(-passed).at[sink].add(passed)
    members = jnp.searchsorted(jnp.cumsum(tallies), jnp.arange(rows * top), side="right").astype(jnp.int32)
    listing = members.reshape(top, rows).T
    listing = listing[jax.random.permutation(jax.random.fold_in(own, 1), rows)]
    turn = jax.random.randint(jax.random.fold_in(own, 2), (rows, 1), 0, top)
    return jnp.take_along_axis(listing, (jnp.arange(top)[None, :] + turn) % top, axis=1)


def portions_of(number_of, total, most, slope, full):
    loads = [(1 << 20) // math.isqrt(rank ** slope) + 1 for rank in range(1, number_of + 1)]
    largest = most if full else min(most, max(-(-total // number_of), total * loads[0] // sum(loads)))
    least = 1 if total - largest >= number_of - 1 else 0
    given, spare = [largest] + [least] * (number_of - 1), total - largest - least * (number_of - 1)
    while spare > 0:
        candidates = [i for i in range(1, number_of) if given[i] < largest] or [i for i in range(1, number_of) if given[i] < most]
        whole, budget = sum([loads[i] for i in candidates]), spare
        for i in candidates:
            more = min(most - given[i], max(1, budget * loads[i] // whole), spare)
            given[i] = given[i] + more
            spare = spare - more
    return np.array(given)


def normal_values(key, dims, width, reach, cuts=(), held_as=jnp.bfloat16):
    result = jax.random.normal(key, dims, jnp.float32) * width
    if len(cuts) > 0:
        result = shard_levels(key, dims, cuts, -0.22, 0.18) * result
    return jnp.clip(result, min=-reach, max=reach).astype(held_as)


def setup_inputs(seed: int = 0) -> dict:
    streams_of = jax.random.split(jax.random.key(seed), 8)
    token_ids = set_ends(ranked(streams_of[0], (TOKENS,), VOC, 2), jax.random.fold_in(streams_of[0], 3), 0, VOC - 1).astype(jnp.int32)
    routes_keys = jax.random.split(jax.random.fold_in(streams_of[1], 1), TOKENS // TOKENS)
    routes_turns = jax.random.permutation(jax.random.fold_in(streams_of[1], 3), TOKENS // TOKENS)
    routes = jax.vmap(lambda own, number: shared_out(jax.random.fold_in(streams_of[1], 2), own, number, TOKENS, EXPERTS, TOPK, CAP, 1))(routes_keys, routes_turns).reshape((TOKENS, TOPK))
    gate_weights = jnp.clip(jax.random.uniform(streams_of[2], (TOKENS, TOPK), jnp.float32, 0.2, 1.0), 0.2, 1.0)
    embed_table = normal_values(streams_of[3], (VOC, D), 0.1, 0.59765625, ((0, 8), (1, 4)))
    w_gate = normal_values(streams_of[4], (EXPERTS, D, FF), (D // 64) ** -0.5, 0.5, ((0, 4), (2, 8)))
    w_up = normal_values(streams_of[5], (EXPERTS, D, FF), (D // 64) ** -0.5, 0.5, ((0, 4), (2, 8)))
    w_down = normal_values(streams_of[6], (EXPERTS, FF, D), FF ** -0.5, 0.125, ((0, 4), (1, 8)))
    return {"token_ids": token_ids, "routes": routes, "gate_weights": gate_weights, "embed_table": embed_table, "w_gate": w_gate, "w_up": w_up, "w_down": w_down}


def reference(token_ids, routes, gate_weights, embed_table, w_gate, w_up, w_down):
    embedded = embed_table[token_ids]
    flat_routes = routes.reshape(-1)
    one_hot = (flat_routes[:, None] == jnp.arange(EXPERTS, dtype=jnp.int32)[None, :]).astype(jnp.int32)
    slot_index = jnp.sum((jnp.cumsum(one_hot, axis=0) - one_hot) * one_hot, axis=1).astype(jnp.int32)
    slot_dest = (flat_routes * CAP + slot_index).astype(jnp.int32)
    repeated = jnp.repeat(embedded, TOPK, axis=0)
    buffer = jnp.zeros((EXPERTS * CAP, D), jnp.bfloat16).at[slot_dest].set(repeated)
    buffer = buffer.reshape(EXPERTS, CAP, D)

    def expert(operands):
        rows_in, gate_mat, up_mat, down_mat = operands
        gate_proj = jnp.dot(rows_in, gate_mat, preferred_element_type=jnp.float32)
        up_proj = jnp.dot(rows_in, up_mat, preferred_element_type=jnp.float32)
        hidden = (jax.nn.silu(gate_proj) * up_proj).astype(jnp.bfloat16)
        return jnp.dot(hidden, down_mat, preferred_element_type=jnp.float32)

    expert_out = lax.map(expert, (buffer, w_gate, w_up, w_down))
    picked = expert_out.reshape(EXPERTS * CAP, D)[slot_dest].reshape(TOKENS, TOPK, D)
    moe_out = jnp.sum(picked * gate_weights[:, :, None].astype(jnp.float32), axis=1)
    residual = (embedded.astype(jnp.float32) + moe_out).astype(jnp.bfloat16)
    block_width = D // N_EXPERT

    def add_block(total, block):
        start = (block * block_width).astype(jnp.int32)
        res_block = lax.dynamic_slice_in_dim(residual, start, block_width, 1)
        tab_block = lax.dynamic_slice_in_dim(embed_table, start, block_width, 1)
        part = lax.dot_general(res_block, tab_block, (((1,), (1,)), ((), ())), preferred_element_type=jnp.float32)
        rounded = lax.optimization_barrier(part.astype(jnp.bfloat16))
        return total + rounded.astype(jnp.float32), None

    start_total = jnp.zeros((TOKENS, VOC), jnp.float32)
    logits, unused = lax.scan(add_block, start_total, jnp.arange(N_EXPERT, dtype=jnp.int32))
    return logits.astype(jnp.bfloat16)
```

```python
import functools

import jax
import jax.numpy as jnp
from jax import lax
from jax.experimental import pallas as pl
from jax.experimental.pallas import tpu as pltpu
from jax.sharding import PartitionSpec as P

MESH = pl.DeviceIdType.MESH
GROUP = ("pipe", "vocab")
VMEM_LIMIT = 67043328
LAG, HOP_LAG = 4, 2


def fused_kernel(
    dims, x_ref, share_ref, gate_ref, up_ref, down_ref, table_ref, o_ref,
    gate, up, down, tiles, scatter, mine, emb, paired, landed, summed, spread, res, held, right, left,
    w_sem, t_sem, a_sem, b_sem, c_sem, n_sem, p_sem, d_sem, e_sem, f_sem, g_sem, r_sem, l_sem,
):
    pipes, vocabs, experts, groups, rows, width, tile, steps, buffers = dims
    chips = pipes * vocabs // 2
    size = 2 * chips
    p, v, e = lax.axis_index("pipe"), lax.axis_index("vocab"), lax.axis_index("expert")
    core, chip = p % 2, (p // 2) * vocabs + v
    me = core * chips + chip
    tokens = size * rows
    dest_rows = tokens // experts
    f32 = jnp.float32

    def at_rank(rank):
        on, where = rank // chips, rank % chips
        return {"pipe": (where // vocabs) * 2 + on, "vocab": where % vocabs}

    def remote(src, dst, sems, index, where):
        return pltpu.make_async_remote_copy(
            src_ref=src, dst_ref=dst, send_sem=sems.at[(0,) + index], recv_sem=sems.at[(1,) + index],
            device_id=where, device_id_type=MESH,
        )

    def weight_copies():
        copies = [
            pltpu.make_async_copy(gate_ref, gate, w_sem.at[0]),
            pltpu.make_async_copy(up_ref, up, w_sem.at[1]),
        ]
        for b in range(experts):
            if len(down_ref.shape) == 2:
                src = down_ref.at[:, b * width : (b + 1) * width]
            else:
                src = down_ref.at[b]
            copies.append(pltpu.make_async_copy(src, down.at[b], w_sem.at[2 + b]))
        return copies

    def tile_copy(s):
        t = s % steps
        return pltpu.make_async_copy(
            table_ref.at[pl.ds(pl.multiple_of(t * tile, tile), tile), :],
            tiles.at[s % buffers],
            t_sem.at[s % buffers],
        )

    barrier = pltpu.get_barrier_semaphore()
    for k in range(1, size):
        pl.semaphore_signal(barrier, inc=1, device_id=at_rank((me + k) % size), device_id_type=MESH)
    for k in range(1, experts):
        pl.semaphore_signal(barrier, inc=1, device_id={"expert": (e + k) % experts}, device_id_type=MESH)
    weights = weight_copies()
    for copy in weights:
        copy.start()
    for s in range(buffers - 1):
        tile_copy(s).start()
    pl.semaphore_wait(barrier, size + experts - 2)

    def scatter_copies(k):
        return [
            remote(x_ref.at[k, (me + i) % size], scatter.at[k, i - 1], a_sem, (k, i - 1), at_rank((me + i) % size))
            for i in range(1, size)
        ]

    def spread_copies(k):
        return [
            remote(
                mine.at[k], emb.at[k, e, me], b_sem, (k, i - 1), {"expert": (e + i) % experts}
            )
            for i in range(1, experts)
        ]

    def plane_copies(k, i):
        b = (e + experts - i) % experts
        src = mine.at[k] if i == 0 else emb.at[k, b, me]
        out = [
            remote(src, emb.at[k, b, me], c_sem, (k, i, c - 1), at_rank(core * chips + (chip + c) % chips))
            for c in range(1, chips)
        ]
        near = remote(src, emb.at[k, b, me], n_sem, (k, i, 0), at_rank((1 - core) * chips + chip))
        return out, near

    def passed_copy(k, i, c):
        b = (e + experts - i) % experts
        at = core * chips + (chip + chips - c) % chips
        return remote(emb.at[k, b, at], emb.at[k, b, at], n_sem, (k, i, c), at_rank((1 - core) * chips + chip))

    def pair_copy(k, b):
        return remote(
            emb.at[k, b, pl.ds((1 - core) * chips, chips)], paired.at[k, b], p_sem, (k, b),
            at_rank((1 - core) * chips + chip),
        )

    def reduce_copies(k, b):
        out = []
        for c in range(1, chips):
            to = core * chips + (chip + c) % chips
            out.append(remote(emb.at[k, b, to], landed.at[k, c - 1, b], d_sem, (k, b, c - 1), at_rank(to)))
        return out

    def expert_copies(k):
        return [
            remote(
                summed.at[k, (e + i) % experts], spread.at[k, i - 1], e_sem, (k, i - 1),
                {"expert": (e + i) % experts},
            )
            for i in range(1, experts)
        ]

    def residual_copies(k):
        out = [
            remote(res.at[k, me], res.at[k, me], f_sem, (k, c - 1), at_rank(core * chips + (chip + c) % chips))
            for c in range(1, chips)
        ]
        near = remote(res.at[k, me], res.at[k, me], g_sem, (k, 0), at_rank((1 - core) * chips + chip))
        return out, near

    def residual_passed(k, c):
        at = core * chips + (chip + chips - c) % chips
        return remote(res.at[k, at], res.at[k, at], g_sem, (k, c), at_rank((1 - core) * chips + chip))

    def start_scatter(k):
        for copy in scatter_copies(k):
            copy.start()

    def own_rows(k):
        total = x_ref[k, me].astype(f32)
        for copy in scatter_copies(k):
            copy.wait_recv()
        for i in range(size - 1):
            total = total + scatter[k, i].astype(f32)
        value = total.astype(mine.dtype)
        mine[k] = value
        emb[k, e, me] = value
        for copy in spread_copies(k):
            copy.start()
        out, near = plane_copies(k, 0)
        for copy in out:
            copy.start()
        near.start()

    def gather_rows(k):
        spreads = spread_copies(k)
        for i in range(1, experts):
            spreads[i - 1].wait_recv()
            out, near = plane_copies(k, i)
            for copy in out:
                copy.start()
            near.start()

    def pass_rows(k):
        for i in range(experts):
            out, _ = plane_copies(k, i)
            for c in range(1, chips):
                out[c - 1].wait_recv()
                passed_copy(k, i, c).start()

    def expert_layer(k):
        gate_sum = jnp.zeros((tokens, gate.shape[1]), f32)
        up_sum = gate_sum
        for i in range(experts):
            _, near = plane_copies(k, i)
            near.wait_recv()
            for c in range(1, chips):
                passed_copy(k, i, c).wait_recv()
            b = (e + experts - i) % experts
            block = emb[k, b].reshape(tokens, width)
            here = pl.ds(pl.multiple_of(b * width, width), width)
            gate_sum = gate_sum + jnp.dot(block, gate[here, :], preferred_element_type=f32)
            up_sum = up_sum + jnp.dot(block, up[here, :], preferred_element_type=f32)
        hidden = (jax.nn.silu(gate_sum) * up_sum).astype(emb.dtype)
        for copy in spread_copies(k):
            copy.wait_send()
        for i in range(experts):
            out, near = plane_copies(k, i)
            for copy in out:
                copy.wait_send()
            near.wait_send()
            for c in range(1, chips):
                passed_copy(k, i, c).wait_send()
        share = share_ref[k]
        for b in range(experts):
            value = jnp.dot(hidden, down[b], preferred_element_type=f32) * share
            emb[k, b] = value.astype(emb.dtype).reshape(size, rows, width)
            if b > 0:
                pair_copy(k, b - 1).start()
        pair_copy(k, experts - 1).start()

    def merge_pairs(k):
        for b in range(experts):
            pair_copy(k, b).wait_recv()
            for c in range(chips):
                at = core * chips + c
                emb[k, b, at] = (emb[k, b, at].astype(f32) + paired[k, b, c].astype(f32)).astype(emb.dtype)
            for copy in reduce_copies(k, b):
                copy.start()

    def sum_rows(k):
        for i in range(1, experts + 1):
            b = (e + i) % experts
            for copy in reduce_copies(k, b):
                copy.wait_recv()
            total = emb[k, b, me].astype(f32)
            for c in range(chips - 1):
                total = total + landed[k, c, b].astype(f32)
            summed[k, b] = total.astype(summed.dtype)
            if i < experts:
                expert_copies(k)[i - 1].start()

    def residual(k):
        total = summed[k, e].astype(f32)
        for i, copy in enumerate(expert_copies(k)):
            copy.wait_recv()
            total = total + spread[k, i].astype(f32)
        res[k, me] = (total + mine[k].astype(f32)).astype(res.dtype)
        out, near = residual_copies(k)
        for copy in out:
            copy.start()
        near.start()

    def gather_residual(k):
        out, near = residual_copies(k)
        for c in range(1, chips):
            out[c - 1].wait_recv()
            residual_passed(k, c).start()
        near.wait_recv()
        for c in range(1, chips):
            residual_passed(k, c).wait_recv()

    def columns(t):
        return pl.ds(pl.multiple_of(t * tile, tile), tile)

    def right_copy(k, d, t, first):
        src = (held if first else right).at[k, d, :, columns(t)]
        return remote(
            src, right.at[k, d, :, columns(t)], r_sem, (k, d, t), {"expert": (e + 1) % experts}
        )

    def left_copy(k, d, t, first):
        src = (held if first else left).at[k, d, :, columns(t)]
        return remote(
            src, left.at[k, d, :, columns(t)], l_sem, (k, d, t), {"expert": (e + experts - 1) % experts}
        )

    total_steps = groups * steps

    def forward(s):
        at_right = s - LAG - HOP_LAG * (e - 1)

        @pl.when((e > 0) & (at_right >= 0) & (at_right < total_steps))
        def _():
            k, t = at_right // steps, at_right % steps

            @pl.loop(0, experts - 1 - e)
            def _(i):
                d = experts - 1 - i
                right_copy(k, d, t, False).wait_recv()
                cols = columns(t)
                value = right[k, d, :, cols].astype(f32) + held[k, d, :, cols].astype(f32)
                right[k, d, :, cols] = value.astype(right.dtype)
                right_copy(k, d, t, False).start()

        at_left = s - LAG - HOP_LAG * (experts - 2 - e)

        @pl.when((e < experts - 1) & (at_left >= 0) & (at_left < total_steps))
        def _():
            k, t = at_left // steps, at_left % steps

            @pl.loop(0, e)
            def _(d):
                left_copy(k, d, t, False).wait_recv()
                cols = columns(t)
                value = left[k, d, :, cols].astype(f32) + held[k, d, :, cols].astype(f32)
                left[k, d, :, cols] = value.astype(left.dtype)
                left_copy(k, d, t, False).start()

        at_end = s - LAG - HOP_LAG * (experts - 2)

        @pl.when((at_end >= 0) & (at_end < total_steps))
        def _():
            k, t = at_end // steps, at_end % steps
            cols = columns(t)
            out_rows = pl.ds(pl.multiple_of(k * dest_rows, dest_rows), dest_rows)
            own = held[k, e, :, cols].astype(f32)

            @pl.when(e == 0)
            def _():
                left_copy(k, e, t, False).wait_recv()
                o_ref[out_rows, cols] = (own + left[k, e, :, cols].astype(f32)).astype(o_ref.dtype)

            @pl.when(e == experts - 1)
            def _():
                right_copy(k, e, t, False).wait_recv()
                o_ref[out_rows, cols] = (own + right[k, e, :, cols].astype(f32)).astype(o_ref.dtype)

            @pl.when((e > 0) & (e < experts - 1))
            def _():
                right_copy(k, e, t, False).wait_recv()
                left_copy(k, e, t, False).wait_recv()
                total = own + right[k, e, :, cols].astype(f32) + left[k, e, :, cols].astype(f32)
                o_ref[out_rows, cols] = total.astype(o_ref.dtype)

    def logits(k):
        @pl.loop(0, steps)
        def _(t):
            s = k * steps + t

            @pl.when(s + buffers - 1 < total_steps)
            def _():
                tile_copy(s + buffers - 1).start()

            tile_copy(s).wait()
            block = lax.dot_general(
                res[k].reshape(tokens, width), tiles[s % buffers], (((1,), (1,)), ((), ())),
                preferred_element_type=f32,
            ).astype(held.dtype)
            cols = columns(t)
            for d in range(experts):
                held[k, d, :, cols] = block[d * dest_rows : (d + 1) * dest_rows]

            @pl.when(e == 0)
            def _():
                @pl.loop(0, experts - 1)
                def _(i):
                    right_copy(k, experts - 1 - i, t, True).start()

            @pl.when(e == experts - 1)
            def _():
                @pl.loop(0, experts - 1)
                def _(i):
                    left_copy(k, i, t, True).start()

            forward(s)

    for k in range(groups):
        start_scatter(k)
    for k in range(groups):
        own_rows(k)
    for copy in weights:
        copy.wait()
    for k in range(groups):
        gather_rows(k)
    for k in range(groups):
        pass_rows(k)
        expert_layer(k)
        merge_pairs(k)
    for k in range(min(2, groups)):
        sum_rows(k)
    for k in range(groups):
        residual(k)
        gather_residual(k)
        if k > 0 and k + 1 < groups:
            sum_rows(k + 1)
        logits(k)

    @pl.loop(total_steps, total_steps + LAG + HOP_LAG * (experts - 2))
    def _(s):
        forward(s)

    for k in range(groups):
        for copy in scatter_copies(k):
            copy.wait_send()
        for b in range(experts):
            pair_copy(k, b).wait_send()
            for copy in reduce_copies(k, b):
                copy.wait_send()
        for copy in expert_copies(k):
            copy.wait_send()
        out, near = residual_copies(k)
        for copy in out:
            copy.wait_send()
        near.wait_send()
        for c in range(1, chips):
            residual_passed(k, c).wait_send()

    @pl.loop(0, total_steps)
    def _(s):
        k, t = s // steps, s % steps

        @pl.loop(0, experts - 1 - e)
        def _(i):
            right_copy(k, experts - 1 - i, t, True).wait_send()

        @pl.loop(0, e)
        def _(d):
            left_copy(k, d, t, True).wait_send()


def fused(x, share, gate, up, down, table, collective_id):
    pipes, vocabs, experts = (lax.axis_size(axis) for axis in ("pipe", "vocab", "expert"))
    groups, size, rows, width = x.shape
    chips = size // 2
    vocab_rows = table.shape[0]
    part = groups * size * rows // experts
    dest_rows = part // groups
    tile = next(t for t in (1024, 512, 256, 128) if vocab_rows % t == 0)
    steps, buffers = vocab_rows // tile, 3
    hidden = gate.shape[1]
    dims = (pipes, vocabs, experts, groups, rows, width, tile, steps, buffers)
    dma = pltpu.SemaphoreType.DMA
    bf16 = x.dtype
    anywhere = pl.BlockSpec(memory_space=pl.ANY)
    inside = pl.BlockSpec(memory_space=pltpu.VMEM)
    return pl.pallas_call(
        functools.partial(fused_kernel, dims),
        out_shape=jax.ShapeDtypeStruct((part, vocab_rows), bf16),
        in_specs=[inside, inside, anywhere, anywhere, anywhere, anywhere],
        out_specs=inside,
        scratch_shapes=[
            pltpu.VMEM(gate.shape, bf16),
            pltpu.VMEM(up.shape, bf16),
            pltpu.VMEM((experts, hidden, width), bf16),
            pltpu.VMEM((buffers, tile, width), bf16),
            pltpu.VMEM((groups, size - 1, rows, width), bf16),
            pltpu.VMEM((groups, rows, width), bf16),
            pltpu.VMEM((groups, experts, size, rows, width), bf16),
            pltpu.VMEM((groups, experts, chips, rows, width), bf16),
            pltpu.VMEM((groups, chips - 1, experts, rows, width), bf16),
            pltpu.VMEM((groups, experts, rows, width), bf16),
            pltpu.VMEM((groups, experts - 1, rows, width), bf16),
            pltpu.VMEM((groups, size, rows, width), bf16),
            pltpu.VMEM((groups, experts, dest_rows, vocab_rows), bf16),
            pltpu.VMEM((groups, experts, dest_rows, vocab_rows), bf16),
            pltpu.VMEM((groups, experts, dest_rows, vocab_rows), bf16),
            dma((2 + experts,)),
            dma((buffers,)),
            dma((2, groups, size - 1)),
            dma((2, groups, experts - 1)),
            dma((2, groups, experts, chips - 1)),
            dma((2, groups, experts, chips)),
            dma((2, groups, experts)),
            dma((2, groups, experts, chips - 1)),
            dma((2, groups, experts - 1)),
            dma((2, groups, chips - 1)),
            dma((2, groups, chips)),
            dma((2, groups, experts, steps)),
            dma((2, groups, experts, steps)),
        ],
        compiler_params=pltpu.CompilerParams(
            collective_id=collective_id, has_side_effects=True, vmem_limit_bytes=VMEM_LIMIT
        ),
    )(x, share, gate, up, down, table)


def token_groups(tokens, size, experts):
    for groups in (3, 2, 1):
        if tokens % (groups * size * 8) == 0 and tokens % (groups * experts * 8) == 0:
            return groups
    return 1


def per_device(token_ids, routes, gate_weights, embed_table, w_gate, w_up, w_down):
    vocab_rows, width = embed_table.shape
    tokens = routes.shape[0]
    experts = lax.axis_size("expert")
    size = lax.axis_size(GROUP)
    groups = token_groups(tokens, size, experts)
    rows = tokens // groups // size

    def regroup(x):
        split = x.reshape((experts, groups, tokens // groups // experts) + x.shape[1:])
        return jnp.swapaxes(split, 0, 1).reshape(x.shape)

    row_base = lax.axis_index(GROUP) * vocab_rows
    local_ids = regroup(token_ids) - row_base
    in_shard = (local_ids >= 0) & (local_ids < vocab_rows)
    x = embed_table.at[jnp.clip(local_ids, 0, vocab_rows - 1)].get(mode="promise_in_bounds")
    x = jnp.where(in_shard[:, None], x, jnp.zeros_like(x)).reshape(groups, size, rows, width)
    share = jnp.sum(
        jnp.where(routes == lax.axis_index("expert"), gate_weights, 0.0), axis=1, keepdims=True
    )
    share = regroup(share).reshape(groups, size * rows, 1)
    down = w_down[0]
    if width % 128:
        down = down.reshape(down.shape[0], experts, width).transpose(1, 0, 2)
    return fused(x, share, w_gate[0], w_up[0], down, embed_table, 0)


def solution(mesh):
    return jax.shard_map(
        per_device,
        mesh=mesh,
        in_specs=(
            P(),
            P(),
            P(),
            P(GROUP, "expert"),
            P("expert", None, GROUP),
            P("expert", None, GROUP),
            P("expert", GROUP, None),
        ),
        out_specs=P("expert", GROUP),
        check_vma=False,
    )
```

```python
import functools
import math

import jax
import jax.numpy as jnp
from jax import lax
from jax.experimental import pallas as pl
from jax.experimental.pallas import tpu as pltpu
from jax.sharding import PartitionSpec as P

MESH = pl.DeviceIdType.MESH
GROUP = ("pipe", "vocab")
VMEM_LIMIT, VMEM_ROOM, VMEM_SPARE = 67043328, 13 * 2**20, 8 * 2**20
LAG, HOP_LAG = 6, 2


def fused_kernel(
    dims, x_ref, share_ref, gate_ref, up_ref, down_ref, table_ref, o_ref,
    gate, up, down, tiles, scatter, mine, emb, paired, landed, summed, spread, res, held, right, left,
    w_sem, t_sem, a_sem, b_sem, c_sem, n_sem, p_sem, d_sem, e_sem, f_sem, g_sem, x_sem, sent_rows, sent,
):
    pipes, vocabs, experts, groups, rows, width, tile, steps, buffers = dims
    chips = pipes * vocabs // 2
    size = 2 * chips
    p, v, e = lax.axis_index("pipe"), lax.axis_index("vocab"), lax.axis_index("expert")
    core, chip = p % 2, (p // 2) * vocabs + v
    me = core * chips + chip
    tokens = size * rows
    dest_rows = tokens // experts
    f32 = jnp.float32

    def at_rank(rank):
        on, where = rank // chips, rank % chips
        return {"pipe": (where // vocabs) * 2 + on, "vocab": where % vocabs}

    def remote(src, dst, send_sem, recv_sem, where):
        return pltpu.make_async_remote_copy(
            src_ref=src, dst_ref=dst, send_sem=send_sem, recv_sem=recv_sem,
            device_id=where, device_id_type=MESH,
        )

    def settle(ref, sem):
        pltpu.make_async_copy(ref, ref, sem).wait()

    def weight_copies():
        copies = [
            pltpu.make_async_copy(gate_ref, gate, w_sem.at[0]),
            pltpu.make_async_copy(up_ref, up, w_sem.at[1]),
        ]
        for b in range(experts):
            if len(down_ref.shape) == 2:
                src = down_ref.at[:, b * width : (b + 1) * width]
            else:
                src = down_ref.at[b]
            copies.append(pltpu.make_async_copy(src, down.at[b], w_sem.at[2]))
        return copies

    def tile_copy(s):
        t = s % steps
        return pltpu.make_async_copy(
            table_ref.at[pl.ds(pl.multiple_of(t * tile, tile), tile), :],
            tiles.at[s % buffers],
            t_sem.at[s % buffers],
        )

    barrier = pltpu.get_barrier_semaphore()
    for k in range(1, size):
        pl.semaphore_signal(barrier, inc=1, device_id=at_rank((me + k) % size), device_id_type=MESH)
    for k in range(1, experts):
        pl.semaphore_signal(barrier, inc=1, device_id={"expert": (e + k) % experts}, device_id_type=MESH)
    weights = weight_copies()
    for copy in weights:
        copy.start()
    for s in range(buffers - 1):
        tile_copy(s).start()
    pl.semaphore_wait(barrier, size + experts - 2)

    partner = at_rank((1 - core) * chips + chip)

    def same_core(c):
        return core * chips + (chip + c) % chips

    def start_scatter(k):
        for i in range(1, size):
            to = (me + i) % size
            remote(x_ref.at[k, to], scatter.at[k, i - 1], sent.at[0], a_sem.at[k], at_rank(to)).start()

    def send_plane(k, i):
        b = (e + experts - i) % experts
        src = mine.at[k] if i == 0 else emb.at[k, b, me]
        for c in range(1, chips):
            remote(src, emb.at[k, b, me], sent_rows.at[k], c_sem.at[k, i], at_rank(same_core(c))).start()
        remote(src, emb.at[k, b, me], sent_rows.at[k], n_sem.at[k, i], partner).start()

    def own_rows(k):
        total = x_ref[k, me].astype(f32)
        settle(scatter.at[k], a_sem.at[k])
        for i in range(size - 1):
            total = total + scatter[k, i].astype(f32)
        value = total.astype(mine.dtype)
        mine[k] = value
        emb[k, e, me] = value
        for i in range(1, experts):
            remote(
                mine.at[k], emb.at[k, e, me], sent.at[1], b_sem.at[k, i - 1], {"expert": (e + i) % experts}
            ).start()
        send_plane(k, 0)

    def gather_rows(k):
        for i in range(1, experts):
            b = (e + experts - i) % experts
            settle(emb.at[k, b, me], b_sem.at[k, i - 1])
            send_plane(k, i)

    def pass_rows(k):
        for i in range(experts):
            b = (e + experts - i) % experts
            settle(emb.at[k, b, pl.ds(0, chips - 1)], c_sem.at[k, i])
            for c in range(1, chips):
                block = emb.at[k, b, same_core(c)]
                remote(block, block, sent_rows.at[k], n_sem.at[k, i], partner).start()

    def expert_layer(k):
        gate_sum = jnp.zeros((tokens, gate.shape[1]), f32)
        up_sum = gate_sum
        for i in range(experts):
            b = (e + experts - i) % experts
            settle(emb.at[k, b, pl.ds(0, chips)], n_sem.at[k, i])
            block = emb[k, b].reshape(tokens, width)
            here = pl.ds(pl.multiple_of(b * width, width), width)
            gate_sum = gate_sum + jnp.dot(block, gate[here, :], preferred_element_type=f32)
            up_sum = up_sum + jnp.dot(block, up[here, :], preferred_element_type=f32)
        hidden = (jax.nn.silu(gate_sum) * up_sum).astype(emb.dtype)
        settle(emb.at[k, :, pl.ds(0, size - 1)], sent_rows.at[k])
        share = share_ref[k]

        def send_pair(b):
            away = emb.at[k, b, pl.ds((1 - core) * chips, chips)]
            remote(away, paired.at[k, b], sent.at[2], p_sem.at[k, b], partner).start()

        for b in range(experts):
            value = jnp.dot(hidden, down[b], preferred_element_type=f32) * share
            emb[k, b] = value.astype(emb.dtype).reshape(size, rows, width)
            if b > 0:
                send_pair(b - 1)
        send_pair(experts - 1)

    def merge_pairs(k):
        for b in range(experts):
            settle(paired.at[k, b], p_sem.at[k, b])
            for c in range(chips):
                at = core * chips + c
                emb[k, b, at] = (emb[k, b, at].astype(f32) + paired[k, b, c].astype(f32)).astype(emb.dtype)
            for c in range(1, chips):
                to = same_core(c)
                remote(emb.at[k, b, to], landed.at[k, b, c - 1], sent.at[3], d_sem.at[k, b], at_rank(to)).start()

    def sum_rows(k):
        for i in range(1, experts + 1):
            b = (e + i) % experts
            settle(landed.at[k, b], d_sem.at[k, b])
            total = emb[k, b, me].astype(f32)
            for c in range(chips - 1):
                total = total + landed[k, b, c].astype(f32)
            summed[k, b] = total.astype(summed.dtype)
            if i < experts:
                remote(summed.at[k, b], spread.at[k, i - 1], sent.at[4], e_sem.at[k], {"expert": b}).start()

    def residual(k):
        total = summed[k, e].astype(f32)
        settle(spread.at[k], e_sem.at[k])
        for i in range(experts - 1):
            total = total + spread[k, i].astype(f32)
        res[k, me] = (total + mine[k].astype(f32)).astype(res.dtype)
        block = res.at[k, me]
        for c in range(1, chips):
            remote(block, block, sent.at[5], f_sem.at[k], at_rank(same_core(c))).start()
        remote(block, block, sent.at[5], g_sem.at[k], partner).start()

    def gather_residual(k):
        settle(res.at[k, pl.ds(0, chips - 1)], f_sem.at[k])
        for c in range(1, chips):
            block = res.at[k, same_core(c)]
            remote(block, block, sent.at[5], g_sem.at[k], partner).start()

    def whole_residual(k):
        settle(res.at[k, pl.ds(0, chips)], g_sem.at[k])

    def columns(t):
        return pl.ds(pl.multiple_of(t * tile, tile), tile)

    def right_copy(k, d, t, first):
        src = (held if first else right).at[k, d, :, columns(t)]
        return remote(
            src, right.at[k, d, :, columns(t)], sent.at[6], x_sem.at[k, d + 1, t], {"expert": (e + 1) % experts}
        )

    def left_copy(k, d, t, first):
        src = (held if first else left).at[k, d, :, columns(t)]
        return remote(
            src, left.at[k, d, :, columns(t)], sent.at[6], x_sem.at[k, d, t], {"expert": (e + experts - 1) % experts}
        )

    total_steps = groups * steps
    last = groups - 1
    early_steps = last * steps
    last_rounds = max(1, experts - 2)

    def add_right(k, d, t):
        right_copy(k, d, t, False).wait_recv()
        cols = columns(t)
        value = right[k, d, :, cols].astype(f32) + held[k, d, :, cols].astype(f32)
        right[k, d, :, cols] = value.astype(right.dtype)
        right_copy(k, d, t, False).start()

    def add_left(k, d, t):
        left_copy(k, d, t, False).wait_recv()
        cols = columns(t)
        value = left[k, d, :, cols].astype(f32) + held[k, d, :, cols].astype(f32)
        left[k, d, :, cols] = value.astype(left.dtype)
        left_copy(k, d, t, False).start()

    def forward(s):
        at_right = s - LAG - HOP_LAG * (e - 1)

        @pl.when((e > 0) & (at_right >= 0) & (at_right < total_steps))
        def _():
            @pl.loop(0, experts - 1 - e)
            def _(i):
                add_right(at_right // steps, experts - 1 - i, at_right % steps)

        at_left = s - LAG - HOP_LAG * (experts - 2 - e)

        @pl.when((e < experts - 1) & (at_left >= 0) & (at_left < total_steps))
        def _():
            @pl.loop(0, e)
            def _(d):
                add_left(at_left // steps, d, at_left % steps)

        at_end = s - LAG - HOP_LAG * (experts - 2)

        @pl.when((at_end >= 0) & (at_end < early_steps))
        def _():
            finish(at_end // steps, at_end % steps)

    def finish(k, t):
        cols = columns(t)
        out_rows = pl.ds(pl.multiple_of(k * dest_rows, dest_rows), dest_rows)
        own = held[k, e, :, cols].astype(f32)

        @pl.when(e == 0)
        def _():
            left_copy(k, e, t, False).wait_recv()
            o_ref[out_rows, cols] = (own + left[k, e, :, cols].astype(f32)).astype(o_ref.dtype)

        @pl.when(e == experts - 1)
        def _():
            right_copy(k, e, t, False).wait_recv()
            o_ref[out_rows, cols] = (own + right[k, e, :, cols].astype(f32)).astype(o_ref.dtype)

        @pl.when((e > 0) & (e < experts - 1))
        def _():
            right_copy(k, e, t, False).wait_recv()
            left_copy(k, e, t, False).wait_recv()
            total = own + right[k, e, :, cols].astype(f32) + left[k, e, :, cols].astype(f32)
            o_ref[out_rows, cols] = total.astype(o_ref.dtype)

    def logits(k):
        @pl.loop(0, steps)
        def _(t):
            s = k * steps + t

            @pl.when(s + buffers - 1 < total_steps)
            def _():
                tile_copy(s + buffers - 1).start()

            tile_copy(s).wait()
            block = lax.dot_general(
                res[k].reshape(tokens, width), tiles[s % buffers], (((1,), (1,)), ((), ())),
                preferred_element_type=f32,
            ).astype(held.dtype)
            cols = columns(t)
            for d in range(experts):
                held[k, d, :, cols] = block[d * dest_rows : (d + 1) * dest_rows]

            rounds = last_rounds if k == last else experts - 1

            @pl.when(e == 0)
            def _():
                @pl.loop(0, rounds)
                def _(i):
                    right_copy(k, experts - 1 - i, t, True).start()

            @pl.when(e == experts - 1)
            def _():
                @pl.loop(0, rounds)
                def _(i):
                    left_copy(k, i, t, True).start()

            forward(s)

    def run(phase, k):
        with jax.named_scope(phase.__name__ + str(k)):
            phase(k)

    first = min(2, groups)
    for k in range(first):
        run(start_scatter, k)
    run(own_rows, 0)
    for k in range(first, groups):
        run(start_scatter, k)
    for k in range(1, first):
        run(own_rows, k)
    run(gather_rows, 0)
    for k in range(first, groups):
        run(own_rows, k)
    for k in range(1, first):
        run(gather_rows, k)
    settle(gate, w_sem.at[0])
    settle(up, w_sem.at[1])
    settle(down, w_sem.at[2])
    run(pass_rows, 0)
    run(expert_layer, 0)
    run(merge_pairs, 0)
    for k in range(first, groups):
        run(gather_rows, k)
    for k in range(1, first):
        run(pass_rows, k)
        run(expert_layer, k)
        run(merge_pairs, k)
    run(sum_rows, 0)
    for k in range(first, groups):
        run(pass_rows, k)
    run(residual, 0)
    for k in range(first, groups):
        run(expert_layer, k)
    run(gather_residual, 0)
    for k in range(first, groups):
        run(merge_pairs, k)
    for k in range(1, first):
        run(sum_rows, k)
    for k in range(groups):
        if k > 0:
            run(residual, k)
            run(gather_residual, k)
        run(whole_residual, k)
        if k > 0 and k + 1 < groups:
            run(sum_rows, k + 1)
        run(logits, k)

    @pl.when(e == 0)
    def _():
        @pl.loop(last_rounds * steps, (experts - 1) * steps)
        def _(j):
            right_copy(last, experts - 1 - j // steps, j % steps, True).start()

    @pl.when(e == experts - 1)
    def _():
        @pl.loop(last_rounds * steps, (experts - 1) * steps)
        def _(j):
            left_copy(last, j // steps, j % steps, True).start()

    @pl.loop(total_steps, total_steps + LAG + HOP_LAG * (experts - 2))
    def _(s):
        with jax.named_scope("epi"):
            forward(s)

    with jax.named_scope("last"):
        @pl.loop(0, steps)
        def _(t):
            finish(last, t)

    settle(scatter, sent.at[0])
    settle(spread, sent.at[1])
    settle(paired, sent.at[2])
    settle(landed, sent.at[3])
    settle(spread, sent.at[4])
    settle(res.at[:, pl.ds(0, size - 1)], sent.at[5])
    settle(held.at[:, pl.ds(0, experts - 1)], sent.at[6])


def fused(x, share, gate, up, down, table, collective_id):
    pipes, vocabs, experts = (lax.axis_size(axis) for axis in ("pipe", "vocab", "expert"))
    groups, size, rows, width = x.shape
    chips = size // 2
    vocab_rows = table.shape[0]
    part = groups * size * rows // experts
    dest_rows = part // groups
    tile = next(t for t in (1024, 512, 256, 128) if vocab_rows % t == 0)
    steps, buffers = vocab_rows // tile, 3
    hidden = gate.shape[1]
    dims = (pipes, vocabs, experts, groups, rows, width, tile, steps, buffers)
    dma = pltpu.SemaphoreType.DMA
    bf16 = x.dtype
    away = pl.BlockSpec(memory_space=pl.ANY)
    inside = pl.BlockSpec(memory_space=pltpu.VMEM)
    buffered = [
        gate.shape,
        up.shape,
        (experts, hidden, width),
        (buffers, tile, width),
        (groups, size - 1, rows, width),
        (groups, rows, width),
        (groups, experts, size, rows, width),
        (groups, experts, chips, rows, width),
        (groups, experts, chips - 1, rows, width),
        (groups, experts, rows, width),
        (groups, experts - 1, rows, width),
        (groups, size, rows, width),
        (groups, experts, dest_rows, vocab_rows),
        (groups, experts, dest_rows, vocab_rows),
        (groups, experts, dest_rows, vocab_rows),
    ]
    held = sum(2 * math.prod(shape[:-1]) * -(-shape[-1] // 128) * 128 for shape in buffered)
    return pl.pallas_call(
        functools.partial(fused_kernel, dims),
        out_shape=jax.ShapeDtypeStruct((part, vocab_rows), bf16),
        in_specs=[inside, inside, away, away, away, away],
        out_specs=inside,
        scratch_shapes=[pltpu.VMEM(shape, bf16) for shape in buffered] + [
            dma((3,)),
            dma((buffers,)),
            dma((groups,)),
            dma((groups, experts - 1)),
            dma((groups, experts)),
            dma((groups, experts)),
            dma((groups, experts)),
            dma((groups, experts)),
            dma((groups,)),
            dma((groups,)),
            dma((groups,)),
            dma((groups, experts + 1, steps)),
            dma((groups,)),
            dma((7,)),
        ],
        compiler_params=pltpu.CompilerParams(
            collective_id=collective_id, has_side_effects=True,
            vmem_limit_bytes=min(VMEM_LIMIT, max(VMEM_LIMIT - VMEM_ROOM, held + VMEM_SPARE)),
        ),
    )(x, share, gate, up, down, table)


def gather_kernel(dims, ids_ref, lane_ids_ref, routes_ref, weights_ref, table_ref, x_ref, share_ref, fetched, sem):
    groups, size, rows, experts, block = dims
    tokens = ids_ref.shape[0]
    width = table_ref.shape[1]
    each = tokens // groups
    dest_rows = each // experts
    shard_rows = table_ref.shape[0]
    base = (lax.axis_index("pipe") * lax.axis_size("vocab") + lax.axis_index("vocab")) * shard_rows

    @pl.loop(0, tokens, unroll=8)
    def _(t):
        row = ids_ref[t] - base
        row = jnp.where((row >= 0) & (row < shard_rows), row, t * block)
        first = pl.multiple_of((row // block) * block, block)
        pltpu.make_async_copy(
            table_ref.at[pl.ds(first, block), :], fetched.at[pl.ds(pl.multiple_of(t * block, block), block), :], sem
        ).start()

    across = lax.broadcasted_iota(jnp.int32, (tokens, tokens), 1)
    along = lax.broadcasted_iota(jnp.int32, (tokens, tokens), 0)
    share = jnp.sum(
        jnp.where(routes_ref[...] == lax.axis_index("expert"), weights_ref[...], 0.0), axis=0, keepdims=True
    )
    share = jnp.sum(jnp.where(across == along, share, 0.0), axis=1, keepdims=True)
    local = jnp.sum(jnp.where(across == along, lane_ids_ref[...], 0), axis=1, keepdims=True) - base
    present = (local >= 0) & (local < shard_rows)
    place = lax.broadcasted_iota(jnp.int32, (tokens, 1), 0) * block + local % block
    place = jnp.where(present, place, -1)
    for k in range(groups):
        for d in range(experts):
            at = (d * groups + k) * dest_rows
            share_ref[k, d * dest_rows : (d + 1) * dest_rows, :] = share[at : at + dest_rows]
    pltpu.make_async_copy(fetched, fetched, sem).wait()
    spots = lax.broadcasted_iota(jnp.int32, (dest_rows, dest_rows * block), 1)
    for k in range(groups):
        for d in range(experts):
            at = (d * groups + k) * dest_rows
            pick = (spots + at * block == place[at : at + dest_rows]).astype(jnp.float32).astype(x_ref.dtype)
            value = jnp.dot(
                pick, fetched[at * block : (at + dest_rows) * block, :], preferred_element_type=jnp.float32
            ).astype(x_ref.dtype)
            for j in range(0, dest_rows, rows):
                x_ref[k, (d * dest_rows + j) // rows] = value[j : j + rows]


def gather(token_ids, routes, gate_weights, table, groups, size, rows):
    tokens, width = routes.shape[0], table.shape[1]
    block, experts = 8, lax.axis_size("expert")
    inside = pl.BlockSpec(memory_space=pltpu.VMEM)
    return pl.pallas_call(
        functools.partial(gather_kernel, (groups, size, rows, experts, block)),
        out_shape=(
            jax.ShapeDtypeStruct((groups, size, rows, width), table.dtype),
            jax.ShapeDtypeStruct((groups, size * rows, 1), jnp.float32),
        ),
        in_specs=[
            pl.BlockSpec(memory_space=pltpu.SMEM), inside, inside, inside, pl.BlockSpec(memory_space=pl.ANY)
        ],
        out_specs=(inside, inside),
        scratch_shapes=[pltpu.VMEM((tokens * block, width), table.dtype), pltpu.SemaphoreType.DMA],
        compiler_params=pltpu.CompilerParams(vmem_limit_bytes=VMEM_LIMIT - VMEM_ROOM),
    )(token_ids, token_ids.reshape(1, tokens), routes.T, gate_weights.T, table)


def token_groups(tokens, size, experts):
    for groups in (3, 2, 1):
        if tokens % (groups * size * 8) == 0 and tokens % (groups * experts * 8) == 0:
            return groups
    return 1


def per_device(token_ids, routes, gate_weights, embed_table, w_gate, w_up, w_down):
    vocab_rows, width = embed_table.shape
    tokens = routes.shape[0]
    experts = lax.axis_size("expert")
    size = lax.axis_size(GROUP)
    groups = token_groups(tokens, size, experts)
    rows = tokens // groups // size

    x, share = gather(token_ids, routes, gate_weights, embed_table, groups, size, rows)
    down = w_down[0]
    if width % 128:
        down = down.reshape(down.shape[0], experts, width).transpose(1, 0, 2)
    return fused(x, share, w_gate[0], w_up[0], down, embed_table, 0)


def solution(mesh):
    return jax.shard_map(
        per_device,
        mesh=mesh,
        in_specs=(
            P(),
            P(),
            P(),
            P(GROUP, "expert"),
            P("expert", None, GROUP),
            P("expert", None, GROUP),
            P("expert", GROUP, None),
        ),
        out_specs=P("expert", GROUP),
        check_vma=False,
    )
```

```python
import functools
import math

import jax
import jax.numpy as jnp
from jax import lax
from jax.experimental import pallas as pl
from jax.experimental.pallas import tpu as pltpu
from jax.sharding import PartitionSpec as P

MESH = pl.DeviceIdType.MESH
GROUP = ("pipe", "vocab")
VMEM_LIMIT, VMEM_ROOM, VMEM_SPARE = 67043328, 13 * 2**20, 8 * 2**20
LAG, HOP_LAG = 6, 2


def fused_kernel(
    dims, x_ref, share_ref, gate_ref, up_ref, down_ref, table_ref, o_ref,
    gate, up, down, tiles, couple, scatter, mine, emb, paired, landed, summed, spread, res, held, right, left,
    w_sem, t_sem, h_sem, a_sem, b_sem, c_sem, n_sem, p_sem, d_sem, e_sem, f_sem, g_sem, x_sem, sent_rows, sent,
):
    pipes, vocabs, experts, groups, rows, width, tile, steps, buffers = dims
    chips = pipes * vocabs // 2
    size = 2 * chips
    p, v, e = lax.axis_index("pipe"), lax.axis_index("vocab"), lax.axis_index("expert")
    core, chip = p % 2, (p // 2) * vocabs + v
    me = core * chips + chip
    tokens = size * rows
    dest_rows = tokens // experts
    f32 = jnp.float32

    def at_rank(rank):
        on, where = rank // chips, rank % chips
        return {"pipe": (where // vocabs) * 2 + on, "vocab": where % vocabs}

    def remote(src, dst, send_sem, recv_sem, where):
        return pltpu.make_async_remote_copy(
            src_ref=src, dst_ref=dst, send_sem=send_sem, recv_sem=recv_sem,
            device_id=where, device_id_type=MESH,
        )

    def settle(ref, sem):
        pltpu.make_async_copy(ref, ref, sem).wait()

    def weight_copies():
        copies = [
            pltpu.make_async_copy(gate_ref, gate, w_sem.at[0]),
            pltpu.make_async_copy(up_ref, up, w_sem.at[1]),
        ]
        for b in range(experts):
            if len(down_ref.shape) == 2:
                src = down_ref.at[:, b * width : (b + 1) * width]
            else:
                src = down_ref.at[b]
            copies.append(pltpu.make_async_copy(src, down.at[b], w_sem.at[2]))
        return copies

    def tile_copy(s):
        t = s % steps
        return pltpu.make_async_copy(
            table_ref.at[pl.ds(pl.multiple_of(t * tile, tile), tile), :],
            tiles.at[s % buffers],
            t_sem.at[s % buffers],
        )

    barrier = pltpu.get_barrier_semaphore()
    for k in range(1, size):
        pl.semaphore_signal(barrier, inc=1, device_id=at_rank((me + k) % size), device_id_type=MESH)
    for k in range(1, experts):
        pl.semaphore_signal(barrier, inc=1, device_id={"expert": (e + k) % experts}, device_id_type=MESH)
    weights = weight_copies()
    for copy in weights:
        copy.start()
    for s in range(buffers - 1):
        tile_copy(s).start()
    pl.semaphore_wait(barrier, size + experts - 2)

    partner = at_rank((1 - core) * chips + chip)

    def same_core(c):
        return core * chips + (chip + c) % chips

    def start_scatter(k):
        away = x_ref.at[k, pl.ds((1 - core) * chips, chips)]
        remote(away, couple.at[k], sent.at[0], h_sem.at[k], partner).start()

    def merge_scatter(k):
        settle(couple.at[k], h_sem.at[k])
        for c in range(chips):
            couple[k, c] = (couple[k, c].astype(f32) + x_ref[k, core * chips + c].astype(f32)).astype(couple.dtype)
        for c in range(1, chips):
            block = couple.at[k, (chip + c) % chips]
            remote(block, scatter.at[k, c - 1], sent.at[7], a_sem.at[k], at_rank(same_core(c))).start()

    def send_plane(k, i):
        b = (e + experts - i) % experts
        src = mine.at[k] if i == 0 else emb.at[k, b, me]
        for c in range(1, chips):
            remote(src, emb.at[k, b, me], sent_rows.at[k], c_sem.at[k, i], at_rank(same_core(c))).start()
        remote(src, emb.at[k, b, me], sent_rows.at[k], n_sem.at[k, i], partner).start()

    def own_rows(k):
        total = couple[k, chip].astype(f32)
        settle(scatter.at[k], a_sem.at[k])
        for i in range(chips - 1):
            total = total + scatter[k, i].astype(f32)
        value = total.astype(mine.dtype)
        mine[k] = value
        emb[k, e, me] = value
        for i in range(1, experts):
            remote(
                mine.at[k], emb.at[k, e, me], sent.at[1], b_sem.at[k, i - 1], {"expert": (e + i) % experts}
            ).start()
        send_plane(k, 0)

    def gather_rows(k):
        for i in range(1, experts):
            b = (e + experts - i) % experts
            settle(emb.at[k, b, me], b_sem.at[k, i - 1])
            send_plane(k, i)

    def pass_rows(k):
        for i in range(experts):
            b = (e + experts - i) % experts
            settle(emb.at[k, b, pl.ds(0, chips - 1)], c_sem.at[k, i])
            for c in range(1, chips):
                block = emb.at[k, b, same_core(c)]
                remote(block, block, sent_rows.at[k], n_sem.at[k, i], partner).start()

    def expert_layer(k):
        gate_sum = jnp.zeros((tokens, gate.shape[1]), f32)
        up_sum = gate_sum
        for i in range(experts):
            b = (e + experts - i) % experts
            settle(emb.at[k, b, pl.ds(0, chips)], n_sem.at[k, i])
            block = emb[k, b].reshape(tokens, width)
            here = pl.ds(pl.multiple_of(b * width, width), width)
            gate_sum = gate_sum + jnp.dot(block, gate[here, :], preferred_element_type=f32)
            up_sum = up_sum + jnp.dot(block, up[here, :], preferred_element_type=f32)
        hidden = (jax.nn.silu(gate_sum) * up_sum).astype(emb.dtype)
        settle(emb.at[k, :, pl.ds(0, size - 1)], sent_rows.at[k])
        share = share_ref[k]

        def send_pair(b):
            away = emb.at[k, b, pl.ds((1 - core) * chips, chips)]
            remote(away, paired.at[k, b], sent.at[2], p_sem.at[k, b], partner).start()

        for b in range(experts):
            value = jnp.dot(hidden, down[b], preferred_element_type=f32) * share
            emb[k, b] = value.astype(emb.dtype).reshape(size, rows, width)
            if b > 0:
                send_pair(b - 1)
        send_pair(experts - 1)

    def merge_pairs(k):
        for b in range(experts):
            settle(paired.at[k, b], p_sem.at[k, b])
            for c in range(chips):
                at = core * chips + c
                emb[k, b, at] = (emb[k, b, at].astype(f32) + paired[k, b, c].astype(f32)).astype(emb.dtype)
            for c in range(1, chips):
                to = same_core(c)
                remote(emb.at[k, b, to], landed.at[k, b, c - 1], sent.at[3], d_sem.at[k, b], at_rank(to)).start()

    def sum_rows(k):
        for i in range(1, experts + 1):
            b = (e + i) % experts
            settle(landed.at[k, b], d_sem.at[k, b])
            total = emb[k, b, me].astype(f32)
            for c in range(chips - 1):
                total = total + landed[k, b, c].astype(f32)
            summed[k, b] = total.astype(summed.dtype)
            if i < experts:
                remote(summed.at[k, b], spread.at[k, i - 1], sent.at[4], e_sem.at[k], {"expert": b}).start()

    def residual(k):
        total = summed[k, e].astype(f32)
        settle(spread.at[k], e_sem.at[k])
        for i in range(experts - 1):
            total = total + spread[k, i].astype(f32)
        res[k, me] = (total + mine[k].astype(f32)).astype(res.dtype)
        block = res.at[k, me]
        for c in range(1, chips):
            remote(block, block, sent.at[5], f_sem.at[k], at_rank(same_core(c))).start()
        remote(block, block, sent.at[5], g_sem.at[k], partner).start()

    def gather_residual(k):
        settle(res.at[k, pl.ds(0, chips - 1)], f_sem.at[k])
        for c in range(1, chips):
            block = res.at[k, same_core(c)]
            remote(block, block, sent.at[5], g_sem.at[k], partner).start()

    def whole_residual(k):
        settle(res.at[k, pl.ds(0, chips)], g_sem.at[k])

    def columns(t):
        return pl.ds(pl.multiple_of(t * tile, tile), tile)

    def right_copy(k, d, t, first):
        src = (held if first else right).at[k, d, :, columns(t)]
        return remote(
            src, right.at[k, d, :, columns(t)], sent.at[6], x_sem.at[k, d + 1, t], {"expert": (e + 1) % experts}
        )

    def left_copy(k, d, t, first):
        src = (held if first else left).at[k, d, :, columns(t)]
        return remote(
            src, left.at[k, d, :, columns(t)], sent.at[6], x_sem.at[k, d, t], {"expert": (e + experts - 1) % experts}
        )

    total_steps = groups * steps
    last = groups - 1
    early_steps = last * steps
    last_rounds = max(1, experts - 2)

    def add_right(k, d, t):
        right_copy(k, d, t, False).wait_recv()
        cols = columns(t)
        value = right[k, d, :, cols].astype(f32) + held[k, d, :, cols].astype(f32)
        right[k, d, :, cols] = value.astype(right.dtype)
        right_copy(k, d, t, False).start()

    def add_left(k, d, t):
        left_copy(k, d, t, False).wait_recv()
        cols = columns(t)
        value = left[k, d, :, cols].astype(f32) + held[k, d, :, cols].astype(f32)
        left[k, d, :, cols] = value.astype(left.dtype)
        left_copy(k, d, t, False).start()

    def forward(s):
        at_right = s - LAG - HOP_LAG * (e - 1)

        @pl.when((e > 0) & (at_right >= 0) & (at_right < total_steps))
        def _():
            @pl.loop(0, experts - 1 - e)
            def _(i):
                add_right(at_right // steps, experts - 1 - i, at_right % steps)

        at_left = s - LAG - HOP_LAG * (experts - 2 - e)

        @pl.when((e < experts - 1) & (at_left >= 0) & (at_left < total_steps))
        def _():
            @pl.loop(0, e)
            def _(d):
                add_left(at_left // steps, d, at_left % steps)

        at_end = s - LAG - HOP_LAG * (experts - 2)

        @pl.when((at_end >= 0) & (at_end < early_steps))
        def _():
            finish(at_end // steps, at_end % steps)

    def finish(k, t):
        cols = columns(t)
        out_rows = pl.ds(pl.multiple_of(k * dest_rows, dest_rows), dest_rows)
        own = held[k, e, :, cols].astype(f32)

        @pl.when(e == 0)
        def _():
            left_copy(k, e, t, False).wait_recv()
            o_ref[out_rows, cols] = (own + left[k, e, :, cols].astype(f32)).astype(o_ref.dtype)

        @pl.when(e == experts - 1)
        def _():
            right_copy(k, e, t, False).wait_recv()
            o_ref[out_rows, cols] = (own + right[k, e, :, cols].astype(f32)).astype(o_ref.dtype)

        @pl.when((e > 0) & (e < experts - 1))
        def _():
            right_copy(k, e, t, False).wait_recv()
            left_copy(k, e, t, False).wait_recv()
            total = own + right[k, e, :, cols].astype(f32) + left[k, e, :, cols].astype(f32)
            o_ref[out_rows, cols] = total.astype(o_ref.dtype)

    def logits(k):
        @pl.loop(0, steps)
        def _(t):
            s = k * steps + t

            @pl.when(s + buffers - 1 < total_steps)
            def _():
                tile_copy(s + buffers - 1).start()

            tile_copy(s).wait()
            block = lax.dot_general(
                res[k].reshape(tokens, width), tiles[s % buffers], (((1,), (1,)), ((), ())),
                preferred_element_type=f32,
            ).astype(held.dtype)
            cols = columns(t)
            for d in range(experts):
                held[k, d, :, cols] = block[d * dest_rows : (d + 1) * dest_rows]

            rounds = last_rounds if k == last else experts - 1

            @pl.when(e == 0)
            def _():
                @pl.loop(0, rounds)
                def _(i):
                    right_copy(k, experts - 1 - i, t, True).start()

            @pl.when(e == experts - 1)
            def _():
                @pl.loop(0, rounds)
                def _(i):
                    left_copy(k, i, t, True).start()

            forward(s)

    def run(phase, k):
        with jax.named_scope(phase.__name__ + str(k)):
            phase(k)

    first = min(2, groups)
    for k in range(groups):
        run(start_scatter, k)
    for k in range(first):
        run(merge_scatter, k)
    run(own_rows, 0)
    for k in range(first, groups):
        run(merge_scatter, k)
    for k in range(1, first):
        run(own_rows, k)
    run(gather_rows, 0)
    for k in range(first, groups):
        run(own_rows, k)
    for k in range(1, first):
        run(gather_rows, k)
    settle(gate, w_sem.at[0])
    settle(up, w_sem.at[1])
    settle(down, w_sem.at[2])
    run(pass_rows, 0)
    run(expert_layer, 0)
    run(merge_pairs, 0)
    for k in range(first, groups):
        run(gather_rows, k)
    for k in range(1, first):
        run(pass_rows, k)
        run(expert_layer, k)
        run(merge_pairs, k)
    run(sum_rows, 0)
    for k in range(first, groups):
        run(pass_rows, k)
    run(residual, 0)
    for k in range(first, groups):
        run(expert_layer, k)
    run(gather_residual, 0)
    for k in range(first, groups):
        run(merge_pairs, k)
    for k in range(1, first):
        run(sum_rows, k)
    for k in range(groups):
        if k > 0:
            run(residual, k)
            run(gather_residual, k)
        run(whole_residual, k)
        if k > 0 and k + 1 < groups:
            run(sum_rows, k + 1)
        run(logits, k)

    @pl.when(e == 0)
    def _():
        @pl.loop(last_rounds * steps, (experts - 1) * steps)
        def _(j):
            right_copy(last, experts - 1 - j // steps, j % steps, True).start()

    @pl.when(e == experts - 1)
    def _():
        @pl.loop(last_rounds * steps, (experts - 1) * steps)
        def _(j):
            left_copy(last, j // steps, j % steps, True).start()

    @pl.loop(total_steps, total_steps + LAG + HOP_LAG * (experts - 2))
    def _(s):
        with jax.named_scope("epi"):
            forward(s)

    with jax.named_scope("last"):
        @pl.loop(0, steps)
        def _(t):
            finish(last, t)

    settle(couple, sent.at[0])
    settle(scatter, sent.at[7])
    settle(spread, sent.at[1])
    settle(paired, sent.at[2])
    settle(landed, sent.at[3])
    settle(spread, sent.at[4])
    settle(res.at[:, pl.ds(0, size - 1)], sent.at[5])
    settle(held.at[:, pl.ds(0, experts - 1)], sent.at[6])


def fused(x, share, gate, up, down, table, collective_id):
    pipes, vocabs, experts = (lax.axis_size(axis) for axis in ("pipe", "vocab", "expert"))
    groups, size, rows, width = x.shape
    chips = size // 2
    vocab_rows = table.shape[0]
    part = groups * size * rows // experts
    dest_rows = part // groups
    tile = next(t for t in (1024, 512, 256, 128) if vocab_rows % t == 0)
    steps, buffers = vocab_rows // tile, 3
    hidden = gate.shape[1]
    dims = (pipes, vocabs, experts, groups, rows, width, tile, steps, buffers)
    dma = pltpu.SemaphoreType.DMA
    bf16 = x.dtype
    away = pl.BlockSpec(memory_space=pl.ANY)
    inside = pl.BlockSpec(memory_space=pltpu.VMEM)
    buffered = [
        gate.shape,
        up.shape,
        (experts, hidden, width),
        (buffers, tile, width),
        (groups, chips, rows, width),
        (groups, chips - 1, rows, width),
        (groups, rows, width),
        (groups, experts, size, rows, width),
        (groups, experts, chips, rows, width),
        (groups, experts, chips - 1, rows, width),
        (groups, experts, rows, width),
        (groups, experts - 1, rows, width),
        (groups, size, rows, width),
        (groups, experts, dest_rows, vocab_rows),
        (groups, experts, dest_rows, vocab_rows),
        (groups, experts, dest_rows, vocab_rows),
    ]
    held = sum(2 * math.prod(shape[:-1]) * -(-shape[-1] // 128) * 128 for shape in buffered)
    return pl.pallas_call(
        functools.partial(fused_kernel, dims),
        out_shape=jax.ShapeDtypeStruct((part, vocab_rows), bf16),
        in_specs=[inside, inside, away, away, away, away],
        out_specs=inside,
        scratch_shapes=[pltpu.VMEM(shape, bf16) for shape in buffered] + [
            dma((3,)),
            dma((buffers,)),
            dma((groups,)),
            dma((groups,)),
            dma((groups, experts - 1)),
            dma((groups, experts)),
            dma((groups, experts)),
            dma((groups, experts)),
            dma((groups, experts)),
            dma((groups,)),
            dma((groups,)),
            dma((groups,)),
            dma((groups, experts + 1, steps)),
            dma((groups,)),
            dma((8,)),
        ],
        compiler_params=pltpu.CompilerParams(
            collective_id=collective_id, has_side_effects=True,
            vmem_limit_bytes=min(VMEM_LIMIT, max(VMEM_LIMIT - VMEM_ROOM, held + VMEM_SPARE)),
        ),
    )(x, share, gate, up, down, table)


def gather_kernel(dims, ids_ref, lane_ids_ref, lane_share_ref, table_ref, x_ref, share_ref, fetched, sem):
    groups, size, rows, experts, block = dims
    tokens = ids_ref.shape[0]
    width = table_ref.shape[1]
    each = tokens // groups
    dest_rows = each // experts
    shard_rows = table_ref.shape[0]
    base = (lax.axis_index("pipe") * lax.axis_size("vocab") + lax.axis_index("vocab")) * shard_rows

    @pl.loop(0, tokens, unroll=8)
    def _(t):
        row = ids_ref[t] - base
        row = jnp.where((row >= 0) & (row < shard_rows), row, t * block)
        first = pl.multiple_of((row // block) * block, block)
        pltpu.make_async_copy(
            table_ref.at[pl.ds(first, block), :], fetched.at[pl.ds(pl.multiple_of(t * block, block), block), :], sem
        ).start()

    across = lax.broadcasted_iota(jnp.int32, (tokens, tokens), 1)
    along = lax.broadcasted_iota(jnp.int32, (tokens, tokens), 0)
    share = jnp.sum(jnp.where(across == along, lane_share_ref[...], 0.0), axis=1, keepdims=True)
    local = jnp.sum(jnp.where(across == along, lane_ids_ref[...], 0), axis=1, keepdims=True) - base
    present = (local >= 0) & (local < shard_rows)
    place = lax.broadcasted_iota(jnp.int32, (tokens, 1), 0) * block + local % block
    place = jnp.where(present, place, -1)
    for k in range(groups):
        for d in range(experts):
            at = (d * groups + k) * dest_rows
            share_ref[k, d * dest_rows : (d + 1) * dest_rows, :] = share[at : at + dest_rows]
    pltpu.make_async_copy(fetched, fetched, sem).wait()
    spots = lax.broadcasted_iota(jnp.int32, (dest_rows, dest_rows * block), 1)
    for k in range(groups):
        for d in range(experts):
            at = (d * groups + k) * dest_rows
            pick = (spots + at * block == place[at : at + dest_rows]).astype(jnp.float32).astype(x_ref.dtype)
            value = jnp.dot(
                pick, fetched[at * block : (at + dest_rows) * block, :], preferred_element_type=jnp.float32
            ).astype(x_ref.dtype)
            for j in range(0, dest_rows, rows):
                x_ref[k, (d * dest_rows + j) // rows] = value[j : j + rows]


def gather(token_ids, share, table, groups, size, rows):
    tokens, width = token_ids.shape[0], table.shape[1]
    block, experts = 8, lax.axis_size("expert")
    inside = pl.BlockSpec(memory_space=pltpu.VMEM)
    return pl.pallas_call(
        functools.partial(gather_kernel, (groups, size, rows, experts, block)),
        out_shape=(
            jax.ShapeDtypeStruct((groups, size, rows, width), table.dtype),
            jax.ShapeDtypeStruct((groups, size * rows, 1), jnp.float32),
        ),
        in_specs=[
            pl.BlockSpec(memory_space=pltpu.SMEM), inside, inside, pl.BlockSpec(memory_space=pl.ANY)
        ],
        out_specs=(inside, inside),
        scratch_shapes=[pltpu.VMEM((tokens * block, width), table.dtype), pltpu.SemaphoreType.DMA],
        compiler_params=pltpu.CompilerParams(vmem_limit_bytes=VMEM_LIMIT - VMEM_ROOM),
    )(token_ids, token_ids.reshape(1, tokens), share.reshape(1, tokens), table)


def token_groups(tokens, size, experts):
    for groups in (3, 2, 1):
        if tokens % (groups * size * 8) == 0 and tokens % (groups * experts * 8) == 0:
            return groups
    return 1


def per_device(token_ids, routes, gate_weights, embed_table, w_gate, w_up, w_down):
    vocab_rows, width = embed_table.shape
    tokens = routes.shape[0]
    experts = lax.axis_size("expert")
    size = lax.axis_size(GROUP)
    groups = token_groups(tokens, size, experts)
    rows = tokens // groups // size

    share = jnp.sum(jnp.where(routes == lax.axis_index("expert"), gate_weights, 0.0), axis=1)
    x, share = gather(token_ids, share, embed_table, groups, size, rows)
    down = w_down[0]
    if width % 128:
        down = down.reshape(down.shape[0], experts, width).transpose(1, 0, 2)
    return fused(x, share, w_gate[0], w_up[0], down, embed_table, 0)


def solution(mesh):
    return jax.shard_map(
        per_device,
        mesh=mesh,
        in_specs=(
            P(),
            P(),
            P(),
            P(GROUP, "expert"),
            P("expert", None, GROUP),
            P("expert", None, GROUP),
            P("expert", GROUP, None),
        ),
        out_specs=P("expert", GROUP),
        check_vma=False,
    )
```
